32 devices in a mesh: fsdp: 16 (over z, y, x), replica: 2 (over core).
Axes of the slice: x: 2, y: 2, z: 4, core: 2. Of those that a mesh axis runs over, the one named last changes fastest.
Arguments:
- gradients: float32 [2, 4194304], P('replica', 'fsdp'), may hold values from -200 to 200, as said below
- tensor_sizes: int32 [192], replicated, may hold values from 1 to 262144, 4194304 in all
- params: float32 [4194304], P(('fsdp', 'replica')), may hold values from -6 to 6
- first_moment: float32 [4194304], P(('fsdp', 'replica')), may hold values from -6e-06 to 6e-06
- second_moment: float32 [4194304], P(('fsdp', 'replica')), may hold values from 1e-12 to 1e-10
Outputs:
- new_params: float32 [4194304], P(('fsdp', 'replica'))
- new_first: float32 [4194304], P(('fsdp', 'replica'))
- new_second: float32 [4194304], P(('fsdp', 'replica'))
- applied_update: float32 [4194304], P(('fsdp', 'replica'))
The draws below stay inside these ranges and needn't reach their ends.
Inputs may be any that keep to these rules, and one draw needn't show every extreme that they name: `gradients`: every entry lies within -200 to 200, blocks of 131072 positions having different scales.
All inputs are finite; a program needn't handle non-finite values.
Results may differ from the reference program's by a relative error of at most 0.0055.
Values sent between devices are 32-bit elements.
A program may use at most 64 MiB of HBM per device.

```python
import math
import jax
import jax.numpy as jnp
import numpy as np

SHARD = 131072
NTENS = 192
FLAT = 4194304
N_REPLICA = 2


def draw_gradients(key, part):
    noise_key, scale_key = jax.random.split(key)
    noise_part = jnp.clip(jax.random.normal(noise_key, (N_REPLICA, FLAT), jnp.float32), -6.0, 6.0)
    levels = jax.random.uniform(scale_key, (FLAT // SHARD,), jnp.float32, -3.5, 3.5)
    return noise_part * jnp.exp(jnp.repeat(levels, SHARD))[None, :]


def block_levels(rng, extent, cuts, least, largest):
    level, own = 1.0, jax.random.fold_in(rng, 6)
    for position, parts in cuts:
        steps = jnp.exp(jax.random.uniform(jax.random.fold_in(own, position), (parts,), jnp.float32, least / len(cuts), largest / len(cuts)))
        level = level * jnp.repeat(steps, extent[position] // parts).reshape([-1 if axis == position else 1 for axis in range(len(extent))])
    return level


def profile(count, total, most, lean):
    weights = [(1 << 20) // math.isqrt(grade ** lean) + 1 for grade in range(2, count + 1)]
    spare, holding = total - most - (count - 1), [1] * (count - 1)
    while spare > 0:
        candidates = [i for i in range(count - 1) if holding[i] < most]
        pool, budget = sum([weights[i] for i in candidates]), spare
        for i in candidates:
            addition = min(most - holding[i], max(1, budget * weights[i] // pool), spare)
            holding[i] = holding[i] + addition
            spare = spare - addition
    return np.array([most] + holding)


def uneven(own_key, amount, total, most, slope):
    if amount == 2:
        one = jax.random.randint(own_key, (), max(1, total - most), min(most, total - 1) + 1)
        return jnp.stack([one, total - one])
    sizes = jnp.asarray(profile(amount, total, most, slope), jnp.int32)
    couples = (amount - 1) // 2
    donor, receiver = sizes[1:1 + 2 * couples:2], sizes[2:2 + 2 * couples:2]
    margin = jnp.minimum(donor - 1, most - receiver)
    moved = jax.random.randint(jax.random.fold_in(own_key, 1), (couples,), 0, 1 << 20) % (margin + 1)
    sizes = sizes.at[1:1 + 2 * couples:2].set(donor - moved).at[2:2 + 2 * couples:2].set(receiver + moved)
    return sizes[jax.random.permutation(jax.random.fold_in(own_key, 2), amount)]


def normal_values(stream_key, dims, spread, bound, cuts=(), kind=jnp.bfloat16):
    values = jax.random.normal(stream_key, dims, jnp.float32) * spread
    if len(cuts) > 0:
        values = block_levels(stream_key, dims, cuts, -0.22, 0.18) * values
    return jnp.clip(values, min=-bound, max=bound).astype(kind)


def setup_inputs(seed: int = 0) -> dict:
    arg_keys = jax.random.split(jax.random.key(seed), 6)
    return {
        "gradients": draw_gradients(jax.random.fold_in(arg_keys[5], 71), 0),
        "tensor_sizes": uneven(arg_keys[1], NTENS, FLAT, FLAT // 16, 2).astype(jnp.int32),
        "params": normal_values(arg_keys[2], (FLAT,), 1.0, 6.0, ((0, 32),), jnp.float32),
        "first_moment": normal_values(arg_keys[3], (FLAT,), 0.000001, 6.000000212225132e-06, ((0, 32),), jnp.float32),
        "second_moment": jnp.clip(jnp.exp(math.log(1.000000013351432e-10) - 4.6051702 * jax.random.uniform(arg_keys[4], (FLAT,), jnp.float32) ** block_levels(arg_keys[4], (FLAT,), ((0, 32),), -0.2, 0.2)), 9.999999960041972e-13, 1.000000013351432e-10),
    }


def reference(gradients, tensor_sizes, params, first_moment, second_moment):
    grad = jnp.sum(gradients, axis=0) / N_REPLICA
    tensor_ends = jnp.cumsum(tensor_sizes, dtype=jnp.int32)
    positions = jnp.arange(FLAT, dtype=jnp.int32)
    owners = jnp.searchsorted(tensor_ends, positions, side="right").astype(jnp.int32)
    grad_sq = jnp.sum(grad * grad)
    clip_scale = jnp.minimum(1.0, 1.0 / jnp.sqrt(grad_sq))
    clipped = clip_scale * grad
    new_first = 0.9 * first_moment + 0.1 * clipped
    new_second = 0.999 * second_moment + 0.001 * clipped * clipped
    direction = (new_first / (1.0 - 0.9 ** 20)) / (jnp.sqrt(new_second / (1.0 - 0.999 ** 20)) + 1e-8) + 0.01 * params
    param_sq = jax.ops.segment_sum(params * params, owners, num_segments=NTENS)
    update_sq = jax.ops.segment_sum(direction * direction, owners, num_segments=NTENS)
    both_pos = (param_sq > 0) & (update_sq > 0)
    trust = jnp.where(both_pos, jnp.sqrt(param_sq) / jnp.sqrt(jnp.where(both_pos, update_sq, 1.0)), 1.0)
    applied_update = trust[owners] * direction
    new_params = params - 0.01 * applied_update
    return new_params, new_first, new_second, applied_update
```

```python
import functools

import jax
import jax.numpy as jnp
from jax import lax
from jax.experimental import pallas as pl
from jax.experimental.pallas import tpu as pltpu
from jax.sharding import PartitionSpec as P

MESH = pl.DeviceIdType.MESH
LANES = 128
F32 = jnp.float32
BF16 = jnp.bfloat16


def round_up(value, unit):
    return -(-value // unit) * unit


def in_hbm(value):
    return pltpu.with_memory_space_constraint(value, pltpu.HBM)


def split(value):
    high = value.astype(BF16)
    return high, (value - high.astype(F32)).astype(BF16)


def running_ends(sizes_row, tcol, trow):
    low = (sizes_row & 4095).astype(F32)
    high = (sizes_row >> 12).astype(F32)
    sub = lax.broadcasted_iota(jnp.int32, (trow, trow), 0)
    lane = lax.broadcasted_iota(jnp.int32, (trow, trow), 1)

    def column(part):
        return jnp.sum(jnp.where(lane <= sub, part, 0.0), axis=1, keepdims=True)

    def row(part):
        own = jnp.sum(jnp.where(lane == sub, part, 0.0), axis=1, keepdims=True)
        return jnp.sum(jnp.where(sub <= lane, own, 0.0), axis=0, keepdims=True)

    def joined(form):
        return form(low).astype(jnp.int32) + (form(high).astype(jnp.int32) << 12)

    size_col = joined(
        lambda part: jnp.sum(jnp.where(lane == sub, part, 0.0), axis=1, keepdims=True)
    )
    return joined(column)[:tcol], size_col[:tcol], joined(row)


def lamb_kernel(
    fsdp, replica, sizes_ref, grads_ref, params_ref, first_ref, second_ref,
    nf_ref, ns_ref, dir_ref, par_ref, mt_ref, w_ref,
    sizes_pad, own_half, peer_half, got_half, mom1, mom2, mask, parts,
    gather_g, gather_p, gather_u, load_sem, half_send, half_recv, send_sem, recv_sem,
):
    n = fsdp * replica
    rows = par_ref.shape[0]
    tcol = mask.shape[0] // 3
    trow = mt_ref.shape[1] // 3
    f_me = lax.axis_index("fsdp")
    r_me = lax.axis_index("replica")
    me = f_me * replica + r_me
    base = me * (rows * LANES)

    def place(k):
        peer = lax.rem(me + k, n)
        return (lax.div(peer, replica), lax.rem(peer, replica))

    def half(c):
        return grads_ref.at[pl.ds(pl.multiple_of(c * rows, rows), rows)]

    peer_loads = []
    for k in range(1, replica):
        peer_loads.append(
            pltpu.make_async_copy(half(lax.rem(r_me + k, replica)), peer_half.at[k - 1], load_sem.at[4 + k])
        )
    for copy in peer_loads:
        copy.start()
    own_load = pltpu.make_async_copy(half(r_me), own_half, load_sem.at[0])
    par_load = pltpu.make_async_copy(params_ref, par_ref, load_sem.at[1])
    mom1_load = pltpu.make_async_copy(first_ref, mom1, load_sem.at[2])
    mom2_load = pltpu.make_async_copy(second_ref, mom2, load_sem.at[3])
    for copy in (par_load, own_load, mom1_load, mom2_load):
        copy.start()

    barrier = pltpu.get_barrier_semaphore()

    def greet(k, carry):
        pl.semaphore_signal(barrier, inc=1, device_id=place(k), device_id_type=MESH)
        return carry

    lax.fori_loop(1, n, greet, 0)

    sizes_pad[...] = jnp.zeros_like(sizes_pad)
    sizes_pad[:, : sizes_ref.shape[1]] = sizes_ref[...]
    end_col, size_col, end_row = running_ends(sizes_pad[...], tcol, trow)
    sizes_row = sizes_pad[...]
    extent = rows * LANES

    def local(pos):
        return jnp.clip(pos - base, 0, extent)

    sc, ec = local(end_col - size_col), local(end_col)
    sr, er = local(end_row - sizes_row), local(end_row)
    sc_row, ec_row = sc >> 7, ec >> 7
    sr_row, er_row = sr >> 7, er >> 7
    lane = lax.broadcasted_iota(jnp.int32, (tcol, LANES), 1)
    after = lane >= (sc & 127)
    before = lane < (ec & 127)
    same = sc_row == ec_row
    start_w = jnp.where(after & (before | jnp.logical_not(same)), 1.0, 0.0)
    end_w = jnp.where(before & jnp.logical_not(same), 1.0, 0.0)

    def as_mask(cond):
        return jnp.where(cond, 1.0, 0.0).astype(BF16)

    step = 256
    for at in range(0, rows, step):
        r = at + lax.broadcasted_iota(jnp.int32, (tcol, step), 1)
        mask[0:tcol, at : at + step] = as_mask((r > sc_row) & (r < ec_row))
        mask[tcol : 2 * tcol, at : at + step] = as_mask(r == sc_row)
        mask[2 * tcol : 3 * tcol, at : at + step] = as_mask(r == ec_row)

    eye = lax.broadcasted_iota(jnp.int32, (tcol, trow), 0) == lax.broadcasted_iota(
        jnp.int32, (tcol, trow), 1
    )

    def sums_row():
        y = jnp.dot(mask[...], parts[...], preferred_element_type=F32)
        y = y[:, :LANES] + y[:, LANES:]
        total = y[0:tcol] + y[tcol : 2 * tcol] * start_w + y[2 * tcol : 3 * tcol] * end_w
        col = jnp.sum(total, axis=1, keepdims=True)
        return jnp.sum(jnp.where(eye, col, 0.0), axis=0, keepdims=True)

    for copy in peer_loads:
        copy.wait()
    pl.semaphore_wait(barrier, n - 1)

    swaps = []
    for k in range(1, replica):
        swaps.append(
            pltpu.make_async_remote_copy(
                src_ref=peer_half.at[k - 1],
                dst_ref=got_half.at[k - 1],
                send_sem=half_send.at[k - 1],
                recv_sem=half_recv.at[k - 1],
                device_id=(f_me, lax.rem(r_me + k, replica)),
                device_id_type=MESH,
            )
        )
    for copy in swaps:
        copy.start()

    par_load.wait()
    block = 128
    for at in range(0, rows, block):
        p = par_ref[at : at + block]
        high, low = split(p * p)
        parts[at : at + block, :LANES] = high
        parts[at : at + block, LANES:] = low
    gather_p[me] = sums_row()

    def share(buffer, which):
        def send(k, carry):
            pltpu.make_async_remote_copy(
                src_ref=buffer.at[me],
                dst_ref=buffer.at[me],
                send_sem=send_sem.at[which],
                recv_sem=recv_sem.at[which],
                device_id=place(k),
                device_id_type=MESH,
            ).start()
            return carry

        lax.fori_loop(1, n, send, 0)

    def arrive(buffer, which):
        most = buffer.at[pl.ds(0, n - 1)]
        pltpu.make_async_copy(most, most, recv_sem.at[which]).wait()

    def leave(buffer, which):
        most = buffer.at[pl.ds(0, n - 1)]
        pltpu.make_async_copy(most, most, send_sem.at[which]).wait()

    own_load.wait()
    for copy in swaps:
        copy.wait()
    acc = jnp.zeros((8, LANES), F32)
    for at in range(0, rows, block):
        g = own_half[at : at + block]
        for k in range(replica - 1):
            g = g + got_half[k, at : at + block]
        g = g * (1.0 / replica)
        own_half[at : at + block] = g
        acc = acc + jnp.sum((g * g).reshape(block // 8, 8, LANES), axis=0)
    gather_g[me] = jnp.sum(acc, axis=0, keepdims=True)
    share(gather_g, 0)
    share(gather_p, 1)

    for at in range(0, rows, block):
        r = at + lax.broadcasted_iota(jnp.int32, (block, trow), 0)
        mt_ref[at : at + block, 0:trow] = as_mask((r > sr_row) & (r < er_row))
        mt_ref[at : at + block, trow : 2 * trow] = as_mask(r == sr_row)
        mt_ref[at : at + block, 2 * trow : 3 * trow] = as_mask(r == er_row)
    w_ref[...] = jnp.zeros_like(w_ref)

    mom1_load.wait()
    mom2_load.wait()
    arrive(gather_g, 0)
    grad_sq = jnp.sum(jnp.sum(gather_g[...], axis=0), axis=1, keepdims=True)
    clip = jnp.minimum(1.0, 1.0 / jnp.sqrt(grad_sq))
    c1 = 1.0 - 0.9**20
    c2 = 1.0 / (1.0 - 0.999**20)
    for at in range(0, rows, block):
        clipped = own_half[at : at + block] * clip
        nf = 0.9 * mom1[at : at + block] + 0.1 * clipped
        ns = 0.999 * mom2[at : at + block] + 0.001 * clipped * clipped
        nf_ref[at : at + block] = nf
        ns_ref[at : at + block] = ns
        d = nf / (c1 * (jnp.sqrt(ns * c2) + 1e-08)) + 0.01 * par_ref[at : at + block]
        dir_ref[at : at + block] = d
        high, low = split(d * d)
        parts[at : at + block, :LANES] = high
        parts[at : at + block, LANES:] = low
    gather_u[me] = sums_row()
    share(gather_u, 2)
    arrive(gather_p, 1)
    param_sq = jnp.sum(gather_p[...], axis=0)
    arrive(gather_u, 2)
    update_sq = jnp.sum(gather_u[...], axis=0)
    both = (param_sq > 0) & (update_sq > 0)
    trust_row = jnp.where(both, jnp.sqrt(param_sq) / jnp.sqrt(jnp.where(both, update_sq, 1.0)), 1.0)
    trust = jnp.sum(jnp.where(eye, trust_row, 0.0), axis=1, keepdims=True)
    weights = (jnp.broadcast_to(trust, (tcol, LANES)), trust * start_w, trust * end_w)
    for slot, weight in enumerate(weights):
        high, low = split(weight)
        w_ref[slot * trow : slot * trow + tcol, :LANES] = high
        w_ref[slot * trow : slot * trow + tcol, LANES:] = low
    leave(gather_g, 0)
    leave(gather_p, 1)
    leave(gather_u, 2)


def apply_kernel(nf_ref, ns_ref, dir_ref, par_ref, mt_ref, w_ref, np_out, nf_out, ns_out, ap_out,
                 np_buf, ap_buf, sem, chunk_sem):
    rows = dir_ref.shape[0]
    early = [
        pltpu.make_async_copy(nf_ref, nf_out, sem.at[0]),
        pltpu.make_async_copy(ns_ref, ns_out, sem.at[1]),
    ]
    for copy in early:
        copy.start()
    chunks = chunk_sem.shape[1]
    block = rows // chunks
    late = []
    for i in range(chunks):
        part = pl.ds(i * block, block)
        t = jnp.dot(mt_ref[part], w_ref[...], preferred_element_type=F32)
        applied = (t[:, :LANES] + t[:, LANES:]) * dir_ref[part]
        ap_buf[part] = applied
        np_buf[part] = par_ref[part] - 0.01 * applied
        for j, (src, dst) in enumerate(((ap_buf, ap_out), (np_buf, np_out))):
            copy = pltpu.make_async_copy(src.at[part], dst.at[part], chunk_sem.at[j, i])
            copy.start()
            late.append(copy)
    for copy in early + late:
        copy.wait()


def shards(fsdp, replica, gradients, tensor_sizes, params, first_moment, second_moment):
    n = fsdp * replica
    rows = params.shape[0] // LANES
    tcol = round_up(tensor_sizes.shape[0], 16)
    trow = round_up(tensor_sizes.shape[0], LANES)
    hbm = pl.BlockSpec(memory_space=pltpu.HBM)
    vmem = pl.BlockSpec(memory_space=pltpu.VMEM)
    flat = (rows, LANES)
    mids = pl.pallas_call(
        functools.partial(lamb_kernel, fsdp, replica),
        out_shape=[
            pltpu.VMEM(flat, F32),
            pltpu.VMEM(flat, F32),
            pltpu.VMEM(flat, F32),
            pltpu.VMEM(flat, F32),
            pltpu.VMEM((rows, 3 * trow), BF16),
            pltpu.VMEM((3 * trow, 2 * LANES), BF16),
        ],
        in_specs=[vmem, hbm, hbm, hbm, hbm],
        out_specs=[vmem] * 6,
        scratch_shapes=[
            pltpu.VMEM((1, trow), jnp.int32),
            pltpu.VMEM(flat, F32),
            pltpu.VMEM((replica - 1,) + flat, F32),
            pltpu.VMEM((replica - 1,) + flat, F32),
            pltpu.VMEM(flat, F32),
            pltpu.VMEM(flat, F32),
            pltpu.VMEM((3 * tcol, rows), BF16),
            pltpu.VMEM((rows, 2 * LANES), BF16),
            pltpu.VMEM((n, 1, LANES), F32),
            pltpu.VMEM((n, 1, trow), F32),
            pltpu.VMEM((n, 1, trow), F32),
            pltpu.SemaphoreType.DMA((4 + replica,)),
            pltpu.SemaphoreType.DMA((replica - 1,)),
            pltpu.SemaphoreType.DMA((replica - 1,)),
            pltpu.SemaphoreType.DMA((3,)),
            pltpu.SemaphoreType.DMA((3,)),
        ],
        compiler_params=pltpu.CompilerParams(
            collective_id=0, has_side_effects=True, vmem_limit_bytes=24 * 1024 * 1024
        ),
    )(
        tensor_sizes.reshape(1, -1),
        in_hbm(gradients.reshape(replica * rows, LANES)),
        in_hbm(params.reshape(flat)),
        in_hbm(first_moment.reshape(flat)),
        in_hbm(second_moment.reshape(flat)),
    )
    chunks = 4
    outs = pl.pallas_call(
        apply_kernel,
        out_shape=[jax.ShapeDtypeStruct(flat, F32)] * 4,
        in_specs=[vmem] * 6,
        out_specs=[hbm] * 4,
        scratch_shapes=[
            pltpu.VMEM(flat, F32),
            pltpu.VMEM(flat, F32),
            pltpu.SemaphoreType.DMA((2,)),
            pltpu.SemaphoreType.DMA((2, chunks)),
        ],
        compiler_params=pltpu.CompilerParams(vmem_limit_bytes=24 * 1024 * 1024),
    )(*mids)
    return tuple(out.reshape(-1) for out in outs)


def solution(mesh):
    flat = P(("fsdp", "replica"))
    return jax.shard_map(
        functools.partial(shards, mesh.shape["fsdp"], mesh.shape["replica"]),
        mesh=mesh,
        in_specs=(P("replica", "fsdp"), P(), flat, flat, flat),
        out_specs=(flat,) * 4,
        check_vma=False,
    )
```

```python
import functools

import jax
import jax.numpy as jnp
from jax import lax
from jax.experimental import pallas as pl
from jax.experimental.pallas import tpu as pltpu
from jax.sharding import PartitionSpec as P

MESH = pl.DeviceIdType.MESH
LANES = 128
F32 = jnp.float32
BF16 = jnp.bfloat16


def round_up(value, unit):
    return -(-value // unit) * unit


def in_hbm(value):
    return pltpu.with_memory_space_constraint(value, pltpu.HBM)


def split(value):
    high = value.astype(BF16)
    return high, (value - high.astype(F32)).astype(BF16)


def running_ends(sizes_row, tcol, trow):
    low = (sizes_row & 4095).astype(F32)
    high = (sizes_row >> 12).astype(F32)
    sub = lax.broadcasted_iota(jnp.int32, (trow, trow), 0)
    lane = lax.broadcasted_iota(jnp.int32, (trow, trow), 1)

    def column(part):
        return jnp.sum(jnp.where(lane <= sub, part, 0.0), axis=1, keepdims=True)

    def row(part):
        own = jnp.sum(jnp.where(lane == sub, part, 0.0), axis=1, keepdims=True)
        return jnp.sum(jnp.where(sub <= lane, own, 0.0), axis=0, keepdims=True)

    def joined(form):
        return form(low).astype(jnp.int32) + (form(high).astype(jnp.int32) << 12)

    size_col = joined(
        lambda part: jnp.sum(jnp.where(lane == sub, part, 0.0), axis=1, keepdims=True)
    )
    return joined(column)[:tcol], size_col[:tcol], joined(row)


def lamb_kernel(
    fsdp, replica, sizes_ref, grads_ref, params_ref, first_ref, second_ref,
    nf_ref, ns_ref, dir_ref, par_ref, mt_ref, w_ref,
    sizes_in, sizes_pad, own_half, peer_half, got_half, mom1, mom2, mask, parts,
    gather_g, gather_p, gather_u, load_sem, peer_sem, half_send, half_recv, send_sem, recv_sem,
    ready_sem, all_sem,
):
    n = fsdp * replica
    rows = par_ref.shape[0]
    tcol = mask.shape[0] // 3
    trow = mt_ref.shape[1] // 3
    f_me = lax.axis_index("fsdp")
    r_me = lax.axis_index("replica")
    me = f_me * replica + r_me
    base = me * (rows * LANES)
    twin = (f_me, 1 - r_me)
    barrier = pltpu.get_barrier_semaphore()

    def chip(k):
        f = f_me + k
        return jnp.where(f >= fsdp, f - fsdp, f)

    @pl.when(r_me == 0)
    def _():
        pl.semaphore_signal(barrier, inc=1, device_id=twin, device_id_type=MESH)

    pieces = peer_sem.shape[0]
    size = rows // pieces

    def piece(c, i):
        return grads_ref.at[pl.ds(pl.multiple_of(c * rows + i * size, size), size)]

    peer_loads = [
        pltpu.make_async_copy(piece(1 - r_me, i), peer_half.at[pl.ds(i * size, size)], peer_sem.at[i])
        for i in range(pieces)
    ]
    own_load = pltpu.make_async_copy(
        grads_ref.at[pl.ds(pl.multiple_of(r_me * rows, rows), rows)], own_half, load_sem.at[0]
    )
    sizes_load = pltpu.make_async_copy(sizes_ref, sizes_in, load_sem.at[4])
    par_load = pltpu.make_async_copy(params_ref, par_ref, load_sem.at[1])
    mom1_load = pltpu.make_async_copy(first_ref, mom1, load_sem.at[2])
    mom2_load = pltpu.make_async_copy(second_ref, mom2, load_sem.at[3])
    for copy in peer_loads + [own_load, sizes_load, par_load, mom1_load, mom2_load]:
        copy.start()

    @pl.when(r_me == 1)
    def _():
        pl.semaphore_wait(barrier, 1)
        pl.semaphore_signal(ready_sem, inc=1, device_id=twin, device_id_type=MESH)

    @pl.when(r_me == 0)
    def _():
        pl.semaphore_wait(ready_sem, 1)

        def greet(k, carry):
            pl.semaphore_signal(barrier, inc=1, device_id=(chip(k), 0), device_id_type=MESH)
            return carry

        lax.fori_loop(1, fsdp, greet, 0)

    swaps = [
        pltpu.make_async_remote_copy(
            src_ref=peer_half.at[pl.ds(i * size, size)],
            dst_ref=got_half.at[pl.ds(i * size, size)],
            send_sem=half_send.at[i],
            recv_sem=half_recv.at[i],
            device_id=twin,
            device_id_type=MESH,
        )
        for i in range(pieces)
    ]
    for load, copy in zip(peer_loads, swaps):
        load.wait()
        copy.start()

    def share(buffer, which):
        def send(place):
            pltpu.make_async_remote_copy(
                src_ref=buffer.at[me],
                dst_ref=buffer.at[me],
                send_sem=send_sem.at[which],
                recv_sem=recv_sem.at[which],
                device_id=place,
                device_id_type=MESH,
            ).start()

        def send_chip(k, carry):
            for c in range(replica):
                send((chip(k), c))
            return carry

        lax.fori_loop(1, fsdp, send_chip, 0)
        send(twin)

    def arrive(buffer, which):
        most = buffer.at[pl.ds(0, n - 1)]
        pltpu.make_async_copy(most, most, recv_sem.at[which]).wait()

    def leave(buffer, which):
        most = buffer.at[pl.ds(0, n - 1)]
        pltpu.make_async_copy(most, most, send_sem.at[which]).wait()

    block = 128
    own_load.wait()
    acc = jnp.zeros((8, LANES), F32)
    for i in range(pieces):
        swaps[i].wait_recv()
        for at in range(i * size, (i + 1) * size, block):
            g = (own_half[at : at + block] + got_half[at : at + block]) * (1.0 / replica)
            own_half[at : at + block] = g
            acc = acc + jnp.sum((g * g).reshape(block // 8, 8, LANES), axis=0)
    gather_g[me] = jnp.sum(acc, axis=0, keepdims=True)

    @pl.when(r_me == 0)
    def _():
        pl.semaphore_wait(barrier, fsdp - 1)
        pl.semaphore_signal(all_sem, inc=1, device_id=twin, device_id_type=MESH)

    @pl.when(r_me == 1)
    def _():
        pl.semaphore_wait(all_sem, 1)

    share(gather_g, 0)

    sizes_load.wait()
    sizes_pad[...] = jnp.zeros_like(sizes_pad)
    sizes_pad[:, : sizes_in.shape[1]] = sizes_in[...]
    sizes_row = sizes_pad[...]
    end_col, size_col, end_row = running_ends(sizes_row, tcol, trow)
    extent = rows * LANES

    def local(pos):
        return jnp.clip(pos - base, 0, extent)

    sc, ec = local(end_col - size_col), local(end_col)
    sr, er = local(end_row - sizes_row), local(end_row)
    sc_row, ec_row = sc >> 7, ec >> 7
    sr_row, er_row = sr >> 7, er >> 7
    lane = lax.broadcasted_iota(jnp.int32, (tcol, LANES), 1)
    after = lane >= (sc & 127)
    before = lane < (ec & 127)
    same = sc_row == ec_row
    start_w = jnp.where(after & (before | jnp.logical_not(same)), 1.0, 0.0)
    end_w = jnp.where(before & jnp.logical_not(same), 1.0, 0.0)

    def as_mask(cond):
        return jnp.where(cond, 1.0, 0.0).astype(BF16)

    step = 256
    for at in range(0, rows, step):
        r = at + lax.broadcasted_iota(jnp.int32, (tcol, step), 1)
        mask[0:tcol, at : at + step] = as_mask((r > sc_row) & (r < ec_row))
        mask[tcol : 2 * tcol, at : at + step] = as_mask(r == sc_row)
        mask[2 * tcol : 3 * tcol, at : at + step] = as_mask(r == ec_row)

    eye = lax.broadcasted_iota(jnp.int32, (tcol, trow), 0) == lax.broadcasted_iota(
        jnp.int32, (tcol, trow), 1
    )

    def sums_row():
        y = jnp.dot(mask[...], parts[...], preferred_element_type=F32)
        y = y[:, :LANES] + y[:, LANES:]
        total = y[0:tcol] + y[tcol : 2 * tcol] * start_w + y[2 * tcol : 3 * tcol] * end_w
        col = jnp.sum(total, axis=1, keepdims=True)
        return jnp.sum(jnp.where(eye, col, 0.0), axis=0, keepdims=True)

    par_load.wait()
    for at in range(0, rows, block):
        p = par_ref[at : at + block]
        high, low = split(p * p)
        parts[at : at + block, :LANES] = high
        parts[at : at + block, LANES:] = low
    gather_p[me] = sums_row()
    share(gather_p, 1)

    mom1_load.wait()
    mom2_load.wait()
    arrive(gather_g, 0)
    grad_sq = jnp.sum(jnp.sum(gather_g[...], axis=0), axis=1, keepdims=True)
    clip = jnp.minimum(1.0, 1.0 / jnp.sqrt(grad_sq))
    c1 = 1.0 - 0.9**20
    c2 = 1.0 / (1.0 - 0.999**20)
    for at in range(0, rows, block):
        clipped = own_half[at : at + block] * clip
        nf = 0.9 * mom1[at : at + block] + 0.1 * clipped
        ns = 0.999 * mom2[at : at + block] + 0.001 * clipped * clipped
        nf_ref[at : at + block] = nf
        ns_ref[at : at + block] = ns
        d = nf / (c1 * (jnp.sqrt(ns * c2) + 1e-08)) + 0.01 * par_ref[at : at + block]
        dir_ref[at : at + block] = d
        high, low = split(d * d)
        parts[at : at + block, :LANES] = high
        parts[at : at + block, LANES:] = low
    gather_u[me] = sums_row()
    share(gather_u, 2)

    for at in range(0, rows, block):
        r = at + lax.broadcasted_iota(jnp.int32, (block, trow), 0)
        mt_ref[at : at + block, 0:trow] = as_mask((r > sr_row) & (r < er_row))
        mt_ref[at : at + block, trow : 2 * trow] = as_mask(r == sr_row)
        mt_ref[at : at + block, 2 * trow : 3 * trow] = as_mask(r == er_row)
    w_ref[...] = jnp.zeros_like(w_ref)

    arrive(gather_p, 1)
    param_sq = jnp.sum(gather_p[...], axis=0)
    for copy in swaps:
        copy.wait_send()
    leave(gather_g, 0)
    leave(gather_p, 1)
    arrive(gather_u, 2)
    update_sq = jnp.sum(gather_u[...], axis=0)
    both = (param_sq > 0) & (update_sq > 0)
    trust_row = jnp.where(both, jnp.sqrt(param_sq) / jnp.sqrt(jnp.where(both, update_sq, 1.0)), 1.0)
    trust = jnp.sum(jnp.where(eye, trust_row, 0.0), axis=1, keepdims=True)
    weights = (jnp.broadcast_to(trust, (tcol, LANES)), trust * start_w, trust * end_w)
    for slot, weight in enumerate(weights):
        high, low = split(weight)
        w_ref[slot * trow : slot * trow + tcol, :LANES] = high
        w_ref[slot * trow : slot * trow + tcol, LANES:] = low
    leave(gather_u, 2)


def apply_kernel(nf_ref, ns_ref, dir_ref, par_ref, mt_ref, w_ref, np_out, nf_out, ns_out, ap_out,
                 np_buf, ap_buf, sem, chunk_sem):
    rows = dir_ref.shape[0]
    early = [
        pltpu.make_async_copy(nf_ref, nf_out, sem.at[0]),
        pltpu.make_async_copy(ns_ref, ns_out, sem.at[1]),
    ]
    for copy in early:
        copy.start()
    chunks = chunk_sem.shape[1]
    block = rows // chunks
    late = []
    for i in range(chunks):
        part = pl.ds(i * block, block)
        t = jnp.dot(mt_ref[part], w_ref[...], preferred_element_type=F32)
        applied = (t[:, :LANES] + t[:, LANES:]) * dir_ref[part]
        ap_buf[part] = applied
        np_buf[part] = par_ref[part] - 0.01 * applied
        for j, (src, dst) in enumerate(((ap_buf, ap_out), (np_buf, np_out))):
            copy = pltpu.make_async_copy(src.at[part], dst.at[part], chunk_sem.at[j, i])
            copy.start()
            late.append(copy)
    for copy in early + late:
        copy.wait()


def shards(fsdp, replica, gradients, tensor_sizes, params, first_moment, second_moment):
    assert replica == 2
    n = fsdp * replica
    rows = params.shape[0] // LANES
    tcol = round_up(tensor_sizes.shape[0], 16)
    trow = round_up(tensor_sizes.shape[0], LANES)
    hbm = pl.BlockSpec(memory_space=pltpu.HBM)
    vmem = pl.BlockSpec(memory_space=pltpu.VMEM)
    flat = (rows, LANES)
    pieces = 4
    mids = pl.pallas_call(
        functools.partial(lamb_kernel, fsdp, replica),
        out_shape=[
            pltpu.VMEM(flat, F32),
            pltpu.VMEM(flat, F32),
            pltpu.VMEM(flat, F32),
            pltpu.VMEM(flat, F32),
            pltpu.VMEM((rows, 3 * trow), BF16),
            pltpu.VMEM((3 * trow, 2 * LANES), BF16),
        ],
        in_specs=[hbm] * 5,
        out_specs=[vmem] * 6,
        scratch_shapes=[
            pltpu.VMEM((1, tensor_sizes.shape[0]), jnp.int32),
            pltpu.VMEM((1, trow), jnp.int32),
            pltpu.VMEM(flat, F32),
            pltpu.VMEM(flat, F32),
            pltpu.VMEM(flat, F32),
            pltpu.VMEM(flat, F32),
            pltpu.VMEM(flat, F32),
            pltpu.VMEM((3 * tcol, rows), BF16),
            pltpu.VMEM((rows, 2 * LANES), BF16),
            pltpu.VMEM((n, 1, LANES), F32),
            pltpu.VMEM((n, 1, trow), F32),
            pltpu.VMEM((n, 1, trow), F32),
            pltpu.SemaphoreType.DMA((5,)),
            pltpu.SemaphoreType.DMA((pieces,)),
            pltpu.SemaphoreType.DMA((pieces,)),
            pltpu.SemaphoreType.DMA((pieces,)),
            pltpu.SemaphoreType.DMA((3,)),
            pltpu.SemaphoreType.DMA((3,)),
            pltpu.SemaphoreType.REGULAR,
            pltpu.SemaphoreType.REGULAR,
        ],
        compiler_params=pltpu.CompilerParams(
            collective_id=0, has_side_effects=True, vmem_limit_bytes=24 * 1024 * 1024
        ),
    )(
        in_hbm(tensor_sizes.reshape(1, -1)),
        in_hbm(gradients.reshape(replica * rows, LANES)),
        in_hbm(params.reshape(flat)),
        in_hbm(first_moment.reshape(flat)),
        in_hbm(second_moment.reshape(flat)),
    )
    chunks = 4
    outs = pl.pallas_call(
        apply_kernel,
        out_shape=[jax.ShapeDtypeStruct(flat, F32)] * 4,
        in_specs=[vmem] * 6,
        out_specs=[hbm] * 4,
        scratch_shapes=[
            pltpu.VMEM(flat, F32),
            pltpu.VMEM(flat, F32),
            pltpu.SemaphoreType.DMA((2,)),
            pltpu.SemaphoreType.DMA((2, chunks)),
        ],
        compiler_params=pltpu.CompilerParams(vmem_limit_bytes=24 * 1024 * 1024),
    )(*mids)
    return tuple(out.reshape(-1) for out in outs)


def solution(mesh):
    flat = P(("fsdp", "replica"))
    return jax.shard_map(
        functools.partial(shards, mesh.shape["fsdp"], mesh.shape["replica"]),
        mesh=mesh,
        in_specs=(P("replica", "fsdp"), P(), flat, flat, flat),
        out_specs=(flat,) * 4,
        check_vma=False,
    )
```

```python
import functools

import jax
import jax.numpy as jnp
from jax import lax
from jax.experimental import pallas as pl
from jax.experimental.pallas import tpu as pltpu
from jax.sharding import PartitionSpec as P

MESH = pl.DeviceIdType.MESH
LANES = 128
F32 = jnp.float32
BF16 = jnp.bfloat16


def round_up(value, unit):
    return -(-value // unit) * unit


def in_hbm(value):
    return pltpu.with_memory_space_constraint(value, pltpu.HBM)


def split(value):
    high = value.astype(BF16)
    return high, (value - high.astype(F32)).astype(BF16)


def running_ends(sizes_row, tcol, trow):
    low = (sizes_row & 4095).astype(F32)
    high = (sizes_row >> 12).astype(F32)
    sub = lax.broadcasted_iota(jnp.int32, (trow, trow), 0)
    lane = lax.broadcasted_iota(jnp.int32, (trow, trow), 1)

    def column(part):
        return jnp.sum(jnp.where(lane <= sub, part, 0.0), axis=1, keepdims=True)

    def row(part):
        own = jnp.sum(jnp.where(lane == sub, part, 0.0), axis=1, keepdims=True)
        return jnp.sum(jnp.where(sub <= lane, own, 0.0), axis=0, keepdims=True)

    def joined(form):
        return form(low).astype(jnp.int32) + (form(high).astype(jnp.int32) << 12)

    size_col = joined(
        lambda part: jnp.sum(jnp.where(lane == sub, part, 0.0), axis=1, keepdims=True)
    )
    return joined(column)[:tcol], size_col[:tcol], joined(row)


def lamb_kernel(
    fsdp, replica, sizes_ref, grads_ref, params_ref, first_ref, second_ref,
    nf_ref, ns_ref, dir_ref, par_ref, mt_ref, w_ref,
    sizes_in, sizes_pad, own_half, peer_half, got_half, mom1, mom2, mask, parts,
    gather_g, gather_p, gather_u, load_sem, peer_sem, half_send, half_recv, send_sem, recv_sem,
    near_send, near_recv, ready_sem, all_sem,
):
    n = fsdp * replica
    rows = par_ref.shape[0]
    tcol = mask.shape[0] // 3
    trow = mt_ref.shape[1] // 3
    f_me = lax.axis_index("fsdp")
    r_me = lax.axis_index("replica")
    me = f_me * replica + r_me
    base = me * (rows * LANES)
    twin = (f_me, 1 - r_me)
    barrier = pltpu.get_barrier_semaphore()

    def chip(k):
        f = f_me + k
        return jnp.where(f >= fsdp, f - fsdp, f)

    @pl.when(r_me == 0)
    def _():
        pl.semaphore_signal(barrier, inc=1, device_id=twin, device_id_type=MESH)

    pieces = peer_sem.shape[0]
    size = rows // pieces

    def piece(c, i):
        return grads_ref.at[pl.ds(pl.multiple_of(c * rows + i * size, size), size)]

    peer_loads = [
        pltpu.make_async_copy(piece(1 - r_me, i), peer_half.at[pl.ds(i * size, size)], peer_sem.at[i])
        for i in range(pieces)
    ]
    own_load = pltpu.make_async_copy(
        grads_ref.at[pl.ds(pl.multiple_of(r_me * rows, rows), rows)], own_half, load_sem.at[0]
    )
    sizes_load = pltpu.make_async_copy(sizes_ref, sizes_in, load_sem.at[4])
    par_load = pltpu.make_async_copy(params_ref, par_ref, load_sem.at[1])
    mom1_load = pltpu.make_async_copy(first_ref, mom1, load_sem.at[2])
    mom2_load = pltpu.make_async_copy(second_ref, mom2, load_sem.at[3])
    for copy in peer_loads + [own_load, sizes_load, par_load, mom1_load, mom2_load]:
        copy.start()

    @pl.when(r_me == 1)
    def _():
        pl.semaphore_wait(barrier, 1)
        pl.semaphore_signal(ready_sem, inc=1, device_id=twin, device_id_type=MESH)

    @pl.when(r_me == 0)
    def _():
        pl.semaphore_wait(ready_sem, 1)

        def greet(k, carry):
            pl.semaphore_signal(barrier, inc=1, device_id=(chip(k), 0), device_id_type=MESH)
            return carry

        lax.fori_loop(1, fsdp, greet, 0)

    swaps = [
        pltpu.make_async_remote_copy(
            src_ref=peer_half.at[pl.ds(i * size, size)],
            dst_ref=got_half.at[pl.ds(i * size, size)],
            send_sem=half_send.at[i],
            recv_sem=half_recv.at[i],
            device_id=twin,
            device_id_type=MESH,
        )
        for i in range(pieces)
    ]
    for load, copy in zip(peer_loads, swaps):
        load.wait()
        copy.start()

    def share(buffer):
        def send(place):
            pltpu.make_async_remote_copy(
                src_ref=buffer.at[me],
                dst_ref=buffer.at[me],
                send_sem=send_sem,
                recv_sem=recv_sem,
                device_id=place,
                device_id_type=MESH,
            ).start()

        def send_chip(k, carry):
            for c in range(replica):
                send((chip(k), c))
            return carry

        lax.fori_loop(1, fsdp, send_chip, 0)
        send(twin)

    def finish(buffer, sem):
        most = buffer.at[pl.ds(0, n - 1)]
        pltpu.make_async_copy(most, most, sem).wait()

    reach = gather_p.shape[0] // 2
    offsets = [o for o in range(-reach, reach + 1) if o != 0]

    def within(pos):
        return (pos >= 0) & (pos < n)

    def near_copy(buffer, which, o):
        to = jnp.clip(me + o, 0, n - 1)
        return pltpu.make_async_remote_copy(
            src_ref=buffer.at[reach],
            dst_ref=buffer.at[reach - o],
            send_sem=near_send.at[which, o + reach],
            recv_sem=near_recv.at[which, o + reach],
            device_id=(lax.div(to, replica), lax.rem(to, replica)),
            device_id_type=MESH,
        )

    def near_start(buffer, which):
        for o in sorted(offsets, key=abs, reverse=True):
            @pl.when(within(me + o))
            def _():
                near_copy(buffer, which, o).start()

    def near_clear(buffer):
        for o in offsets:
            @pl.when(jnp.logical_not(within(me - o)))
            def _():
                buffer[reach - o] = jnp.zeros(buffer.shape[1:], F32)

    def near_arrive(buffer, which):
        for o in offsets:
            @pl.when(within(me - o))
            def _():
                near_copy(buffer, which, o).wait_recv()

    def near_leave(buffer, which):
        for o in offsets:
            @pl.when(within(me + o))
            def _():
                near_copy(buffer, which, o).wait_send()

    block = 128
    own_load.wait()
    acc = jnp.zeros((8, LANES), F32)
    for i in range(pieces):
        swaps[i].wait_recv()
        for at in range(i * size, (i + 1) * size, block):
            g = (own_half[at : at + block] + got_half[at : at + block]) * (1.0 / replica)
            own_half[at : at + block] = g
            acc = acc + jnp.sum((g * g).reshape(block // 8, 8, LANES), axis=0)
    gather_g[me] = jnp.sum(acc, axis=0, keepdims=True)

    @pl.when(r_me == 0)
    def _():
        pl.semaphore_wait(barrier, fsdp - 1)
        pl.semaphore_signal(all_sem, inc=1, device_id=twin, device_id_type=MESH)

    @pl.when(r_me == 1)
    def _():
        pl.semaphore_wait(all_sem, 1)

    share(gather_g)
    near_clear(gather_p)
    near_clear(gather_u)

    sizes_load.wait()
    sizes_pad[...] = jnp.zeros_like(sizes_pad)
    sizes_pad[:, : sizes_in.shape[1]] = sizes_in[...]
    sizes_row = sizes_pad[...]
    end_col, size_col, end_row = running_ends(sizes_row, tcol, trow)
    extent = rows * LANES

    def local(pos):
        return jnp.clip(pos - base, 0, extent)

    sc, ec = local(end_col - size_col), local(end_col)
    sr, er = local(end_row - sizes_row), local(end_row)
    sc_row, ec_row = sc >> 7, ec >> 7
    sr_row, er_row = sr >> 7, er >> 7
    lane = lax.broadcasted_iota(jnp.int32, (tcol, LANES), 1)
    after = lane >= (sc & 127)
    before = lane < (ec & 127)
    same = sc_row == ec_row
    start_w = jnp.where(after & (before | jnp.logical_not(same)), 1.0, 0.0)
    end_w = jnp.where(before & jnp.logical_not(same), 1.0, 0.0)

    def as_mask(cond):
        return jnp.where(cond, 1.0, 0.0).astype(BF16)

    step = 256
    for at in range(0, rows, step):
        r = at + lax.broadcasted_iota(jnp.int32, (tcol, step), 1)
        mask[0:tcol, at : at + step] = as_mask((r > sc_row) & (r < ec_row))
        mask[tcol : 2 * tcol, at : at + step] = as_mask(r == sc_row)
        mask[2 * tcol : 3 * tcol, at : at + step] = as_mask(r == ec_row)

    eye = lax.broadcasted_iota(jnp.int32, (tcol, trow), 0) == lax.broadcasted_iota(
        jnp.int32, (tcol, trow), 1
    )

    def sums_row():
        y = jnp.dot(mask[...], parts[...], preferred_element_type=F32)
        y = y[:, :LANES] + y[:, LANES:]
        total = y[0:tcol] + y[tcol : 2 * tcol] * start_w + y[2 * tcol : 3 * tcol] * end_w
        col = jnp.sum(total, axis=1, keepdims=True)
        return jnp.sum(jnp.where(eye, col, 0.0), axis=0, keepdims=True)

    par_load.wait()
    for at in range(0, rows, block):
        p = par_ref[at : at + block]
        high, low = split(p * p)
        parts[at : at + block, :LANES] = high
        parts[at : at + block, LANES:] = low
    gather_p[reach] = sums_row()
    near_start(gather_p, 0)

    mom1_load.wait()
    mom2_load.wait()
    finish(gather_g, recv_sem)
    grad_sq = jnp.sum(jnp.sum(gather_g[...], axis=0), axis=1, keepdims=True)
    clip = jnp.minimum(1.0, 1.0 / jnp.sqrt(grad_sq))
    c1 = 1.0 - 0.9**20
    c2 = 1.0 / (1.0 - 0.999**20)
    for at in range(0, rows, block):
        clipped = own_half[at : at + block] * clip
        nf = 0.9 * mom1[at : at + block] + 0.1 * clipped
        ns = 0.999 * mom2[at : at + block] + 0.001 * clipped * clipped
        nf_ref[at : at + block] = nf
        ns_ref[at : at + block] = ns
        d = nf / (c1 * (jnp.sqrt(ns * c2) + 1e-08)) + 0.01 * par_ref[at : at + block]
        dir_ref[at : at + block] = d
        high, low = split(d * d)
        parts[at : at + block, :LANES] = high
        parts[at : at + block, LANES:] = low
    gather_u[reach] = sums_row()
    near_start(gather_u, 1)

    for at in range(0, rows, block):
        r = at + lax.broadcasted_iota(jnp.int32, (block, trow), 0)
        mt_ref[at : at + block, 0:trow] = as_mask((r > sr_row) & (r < er_row))
        mt_ref[at : at + block, trow : 2 * trow] = as_mask(r == sr_row)
        mt_ref[at : at + block, 2 * trow : 3 * trow] = as_mask(r == er_row)
    w_ref[...] = jnp.zeros_like(w_ref)

    near_arrive(gather_p, 0)
    param_sq = jnp.sum(gather_p[...], axis=0)
    for copy in swaps:
        copy.wait_send()
    finish(gather_g, send_sem)
    near_leave(gather_p, 0)
    near_arrive(gather_u, 1)
    update_sq = jnp.sum(gather_u[...], axis=0)
    both = (param_sq > 0) & (update_sq > 0)
    trust_row = jnp.where(both, jnp.sqrt(param_sq) / jnp.sqrt(jnp.where(both, update_sq, 1.0)), 1.0)
    trust = jnp.sum(jnp.where(eye, trust_row, 0.0), axis=1, keepdims=True)
    weights = (jnp.broadcast_to(trust, (tcol, LANES)), trust * start_w, trust * end_w)
    for slot, weight in enumerate(weights):
        high, low = split(weight)
        w_ref[slot * trow : slot * trow + tcol, :LANES] = high
        w_ref[slot * trow : slot * trow + tcol, LANES:] = low
    near_leave(gather_u, 1)


def apply_kernel(nf_ref, ns_ref, dir_ref, par_ref, mt_ref, w_ref, np_out, nf_out, ns_out, ap_out,
                 np_buf, ap_buf, sem, chunk_sem):
    rows = dir_ref.shape[0]
    early = [
        pltpu.make_async_copy(nf_ref, nf_out, sem.at[0]),
        pltpu.make_async_copy(ns_ref, ns_out, sem.at[1]),
    ]
    for copy in early:
        copy.start()
    chunks = chunk_sem.shape[1]
    block = rows // chunks
    late = []
    for i in range(chunks):
        part = pl.ds(i * block, block)
        t = jnp.dot(mt_ref[part], w_ref[...], preferred_element_type=F32)
        applied = (t[:, :LANES] + t[:, LANES:]) * dir_ref[part]
        ap_buf[part] = applied
        np_buf[part] = par_ref[part] - 0.01 * applied
        for j, (src, dst) in enumerate(((ap_buf, ap_out), (np_buf, np_out))):
            copy = pltpu.make_async_copy(src.at[part], dst.at[part], chunk_sem.at[j, i])
            copy.start()
            late.append(copy)
    for copy in early + late:
        copy.wait()


def shards(fsdp, replica, gradients, tensor_sizes, params, first_moment, second_moment):
    assert replica == 2
    n = fsdp * replica
    rows = params.shape[0] // LANES
    tcol = round_up(tensor_sizes.shape[0], 16)
    trow = round_up(tensor_sizes.shape[0], LANES)
    hbm = pl.BlockSpec(memory_space=pltpu.HBM)
    vmem = pl.BlockSpec(memory_space=pltpu.VMEM)
    flat = (rows, LANES)
    pieces = 4
    reach = -(-n // 16)
    mids = pl.pallas_call(
        functools.partial(lamb_kernel, fsdp, replica),
        out_shape=[
            pltpu.VMEM(flat, F32),
            pltpu.VMEM(flat, F32),
            pltpu.VMEM(flat, F32),
            pltpu.VMEM(flat, F32),
            pltpu.VMEM((rows, 3 * trow), BF16),
            pltpu.VMEM((3 * trow, 2 * LANES), BF16),
        ],
        in_specs=[hbm] * 5,
        out_specs=[vmem] * 6,
        scratch_shapes=[
            pltpu.VMEM((1, tensor_sizes.shape[0]), jnp.int32),
            pltpu.VMEM((1, trow), jnp.int32),
            pltpu.VMEM(flat, F32),
            pltpu.VMEM(flat, F32),
            pltpu.VMEM(flat, F32),
            pltpu.VMEM(flat, F32),
            pltpu.VMEM(flat, F32),
            pltpu.VMEM((3 * tcol, rows), BF16),
            pltpu.VMEM((rows, 2 * LANES), BF16),
            pltpu.VMEM((n, 1, LANES), F32),
            pltpu.VMEM((2 * reach + 1, 1, trow), F32),
            pltpu.VMEM((2 * reach + 1, 1, trow), F32),
            pltpu.SemaphoreType.DMA((5,)),
            pltpu.SemaphoreType.DMA((pieces,)),
            pltpu.SemaphoreType.DMA((pieces,)),
            pltpu.SemaphoreType.DMA((pieces,)),
            pltpu.SemaphoreType.DMA,
            pltpu.SemaphoreType.DMA,
            pltpu.SemaphoreType.DMA((2, 2 * reach + 1)),
            pltpu.SemaphoreType.DMA((2, 2 * reach + 1)),
            pltpu.SemaphoreType.REGULAR,
            pltpu.SemaphoreType.REGULAR,
        ],
        compiler_params=pltpu.CompilerParams(
            collective_id=0, has_side_effects=True, vmem_limit_bytes=24 * 1024 * 1024
        ),
    )(
        in_hbm(tensor_sizes.reshape(1, -1)),
        in_hbm(gradients.reshape(replica * rows, LANES)),
        in_hbm(params.reshape(flat)),
        in_hbm(first_moment.reshape(flat)),
        in_hbm(second_moment.reshape(flat)),
    )
    chunks = 4
    outs = pl.pallas_call(
        apply_kernel,
        out_shape=[jax.ShapeDtypeStruct(flat, F32)] * 4,
        in_specs=[vmem] * 6,
        out_specs=[hbm] * 4,
        scratch_shapes=[
            pltpu.VMEM(flat, F32),
            pltpu.VMEM(flat, F32),
            pltpu.SemaphoreType.DMA((2,)),
            pltpu.SemaphoreType.DMA((2, chunks)),
        ],
        compiler_params=pltpu.CompilerParams(vmem_limit_bytes=24 * 1024 * 1024),
    )(*mids)
    return tuple(out.reshape(-1) for out in outs)


def solution(mesh):
    flat = P(("fsdp", "replica"))
    return jax.shard_map(
        functools.partial(shards, mesh.shape["fsdp"], mesh.shape["replica"]),
        mesh=mesh,
        in_specs=(P("replica", "fsdp"), P(), flat, flat, flat),
        out_specs=(flat,) * 4,
        check_vma=False,
    )
```

```python
import functools

import jax
import jax.numpy as jnp
from jax import lax
from jax.experimental import pallas as pl
from jax.experimental.pallas import tpu as pltpu
from jax.sharding import PartitionSpec as P

MESH = pl.DeviceIdType.MESH
LANES = 128
F32 = jnp.float32
BF16 = jnp.bfloat16


def round_up(value, unit):
    return -(-value // unit) * unit


def in_hbm(value):
    return pltpu.with_memory_space_constraint(value, pltpu.HBM)


def split(value):
    high = value.astype(BF16)
    return high, (value - high.astype(F32)).astype(BF16)


def running_ends(sizes_row, tcol, trow):
    low = (sizes_row & 4095).astype(F32)
    high = (sizes_row >> 12).astype(F32)
    sub = lax.broadcasted_iota(jnp.int32, (trow, trow), 0)
    lane = lax.broadcasted_iota(jnp.int32, (trow, trow), 1)

    def column(part):
        return jnp.sum(jnp.where(lane <= sub, part, 0.0), axis=1, keepdims=True)

    def row(part):
        own = jnp.sum(jnp.where(lane == sub, part, 0.0), axis=1, keepdims=True)
        return jnp.sum(jnp.where(sub <= lane, own, 0.0), axis=0, keepdims=True)

    def joined(form):
        return form(low).astype(jnp.int32) + (form(high).astype(jnp.int32) << 12)

    size_col = joined(
        lambda part: jnp.sum(jnp.where(lane == sub, part, 0.0), axis=1, keepdims=True)
    )
    return joined(column)[:tcol], size_col[:tcol], joined(row)


def lamb_kernel(
    fsdp, replica, sizes_ref, grads_ref, params_ref, first_ref, second_ref,
    nf_ref, ns_ref, dir_ref, par_ref, mt_ref, w_ref,
    sizes_in, sizes_pad, own_half, peer_half, got_half, mom1, mom2, mask, parts,
    gather_g, gather_p, gather_u, load_sem, peer_sem, half_send, half_recv, send_sem, recv_sem,
    near_send, near_recv, ready_sem, all_sem,
):
    n = fsdp * replica
    rows = par_ref.shape[0]
    tcol = mask.shape[0] // 3
    trow = mt_ref.shape[1] // 3
    f_me = lax.axis_index("fsdp")
    r_me = lax.axis_index("replica")
    me = f_me * replica + r_me
    base = me * (rows * LANES)
    twin = (f_me, 1 - r_me)
    barrier = pltpu.get_barrier_semaphore()

    def chip(k):
        f = f_me + k
        return jnp.where(f >= fsdp, f - fsdp, f)

    @pl.when(r_me == 0)
    def _():
        pl.semaphore_signal(barrier, inc=1, device_id=twin, device_id_type=MESH)

    pieces = peer_sem.shape[0]
    size = rows // pieces

    def piece(c, i):
        return grads_ref.at[pl.ds(pl.multiple_of(c * rows + i * size, size), size)]

    peer_loads = [
        pltpu.make_async_copy(piece(1 - r_me, i), peer_half.at[pl.ds(i * size, size)], peer_sem.at[i])
        for i in range(pieces)
    ]
    own_load = pltpu.make_async_copy(
        grads_ref.at[pl.ds(pl.multiple_of(r_me * rows, rows), rows)], own_half, load_sem.at[0]
    )
    sizes_load = pltpu.make_async_copy(sizes_ref, sizes_in, load_sem.at[4])
    par_load = pltpu.make_async_copy(params_ref, par_ref, load_sem.at[1])
    mom1_load = pltpu.make_async_copy(first_ref, mom1, load_sem.at[2])
    mom2_load = pltpu.make_async_copy(second_ref, mom2, load_sem.at[3])
    for copy in peer_loads + [own_load, sizes_load, par_load, mom1_load, mom2_load]:
        copy.start()

    @pl.when(r_me == 1)
    def _():
        pl.semaphore_wait(barrier, 1)
        pl.semaphore_signal(ready_sem, inc=1, device_id=twin, device_id_type=MESH)

    @pl.when(r_me == 0)
    def _():
        pl.semaphore_wait(ready_sem, 1)

        def greet(k, carry):
            pl.semaphore_signal(barrier, inc=1, device_id=(chip(k), 0), device_id_type=MESH)
            return carry

        lax.fori_loop(1, fsdp, greet, 0)

    swaps = [
        pltpu.make_async_remote_copy(
            src_ref=peer_half.at[pl.ds(i * size, size)],
            dst_ref=got_half.at[pl.ds(i * size, size)],
            send_sem=half_send.at[i],
            recv_sem=half_recv.at[i],
            device_id=twin,
            device_id_type=MESH,
        )
        for i in range(pieces)
    ]
    for load, copy in zip(peer_loads, swaps):
        load.wait()
        copy.start()

    def share(buffer):
        def send(place):
            pltpu.make_async_remote_copy(
                src_ref=buffer.at[me],
                dst_ref=buffer.at[me],
                send_sem=send_sem,
                recv_sem=recv_sem,
                device_id=place,
                device_id_type=MESH,
            ).start()

        def send_chip(k, carry):
            for c in range(replica):
                send((chip(k), c))
            return carry

        lax.fori_loop(1, fsdp, send_chip, 0)
        send(twin)

    def finish(buffer, sem):
        most = buffer.at[pl.ds(0, n - 1)]
        pltpu.make_async_copy(most, most, sem).wait()

    reach = gather_p.shape[0] // 2
    offsets = [o for o in range(-reach, reach + 1) if o != 0]

    def within(pos):
        return (pos >= 0) & (pos < n)

    def near_copy(buffer, which, o):
        to = jnp.clip(me + o, 0, n - 1)
        return pltpu.make_async_remote_copy(
            src_ref=buffer.at[reach],
            dst_ref=buffer.at[reach - o],
            send_sem=near_send.at[which, o + reach],
            recv_sem=near_recv.at[which, o + reach],
            device_id=(lax.div(to, replica), lax.rem(to, replica)),
            device_id_type=MESH,
        )

    def near_start(buffer, which):
        for o in sorted(offsets, key=abs, reverse=True):
            @pl.when(within(me + o))
            def _():
                near_copy(buffer, which, o).start()

    def near_clear(buffer):
        for o in offsets:
            @pl.when(jnp.logical_not(within(me - o)))
            def _():
                buffer[reach - o] = jnp.zeros(buffer.shape[1:], F32)

    def near_arrive(buffer, which):
        for o in offsets:
            @pl.when(within(me - o))
            def _():
                near_copy(buffer, which, o).wait_recv()

    def near_leave(buffer, which):
        for o in offsets:
            @pl.when(within(me + o))
            def _():
                near_copy(buffer, which, o).wait_send()

    @pl.when(r_me == 0)
    def _():
        pl.semaphore_wait(barrier, fsdp - 1)
        pl.semaphore_signal(all_sem, inc=1, device_id=twin, device_id_type=MESH)

    block = 128
    own_load.wait()
    acc = jnp.zeros((8, LANES), F32)
    for i in range(pieces):
        swaps[i].wait_recv()
        for at in range(i * size, (i + 1) * size, block):
            g = (own_half[at : at + block] + got_half[at : at + block]) * (1.0 / replica)
            own_half[at : at + block] = g
            acc = acc + jnp.sum((g * g).reshape(block // 8, 8, LANES), axis=0)
    gather_g[me] = jnp.sum(acc, axis=0, keepdims=True)

    @pl.when(r_me == 1)
    def _():
        pl.semaphore_wait(all_sem, 1)

    share(gather_g)
    near_clear(gather_p)
    near_clear(gather_u)

    sizes_load.wait()
    sizes_pad[...] = jnp.zeros_like(sizes_pad)
    sizes_pad[:, : sizes_in.shape[1]] = sizes_in[...]
    sizes_row = sizes_pad[...]
    end_col, size_col, end_row = running_ends(sizes_row, tcol, trow)
    extent = rows * LANES

    def local(pos):
        return jnp.clip(pos - base, 0, extent)

    sc, ec = local(end_col - size_col), local(end_col)
    sr, er = local(end_row - sizes_row), local(end_row)
    sc_row, ec_row = sc >> 7, ec >> 7
    sr_row, er_row = sr >> 7, er >> 7
    lane = lax.broadcasted_iota(jnp.int32, (tcol, LANES), 1)
    after = lane >= (sc & 127)
    before = lane < (ec & 127)
    same = sc_row == ec_row
    start_w = jnp.where(after & (before | jnp.logical_not(same)), 1.0, 0.0)
    end_w = jnp.where(before & jnp.logical_not(same), 1.0, 0.0)

    def as_mask(cond):
        return jnp.where(cond, 1.0, 0.0).astype(BF16)

    step = 256
    for at in range(0, rows, step):
        r = at + lax.broadcasted_iota(jnp.int32, (tcol, step), 1)
        mask[0:tcol, at : at + step] = as_mask((r > sc_row) & (r < ec_row))
        mask[tcol : 2 * tcol, at : at + step] = as_mask(r == sc_row)
        mask[2 * tcol : 3 * tcol, at : at + step] = as_mask(r == ec_row)

    eye = lax.broadcasted_iota(jnp.int32, (tcol, trow), 0) == lax.broadcasted_iota(
        jnp.int32, (tcol, trow), 1
    )

    def masked(at, span):
        y = jnp.dot(mask[:, at : at + span], parts[at : at + span], preferred_element_type=F32)
        return y[:, :LANES] + y[:, LANES:]

    def sums_row(y):
        total = y[0:tcol] + y[tcol : 2 * tcol] * start_w + y[2 * tcol : 3 * tcol] * end_w
        col = jnp.sum(total, axis=1, keepdims=True)
        return jnp.sum(jnp.where(eye, col, 0.0), axis=0, keepdims=True)

    par_load.wait()
    for at in range(0, rows, block):
        p = par_ref[at : at + block]
        high, low = split(p * p)
        parts[at : at + block, :LANES] = high
        parts[at : at + block, LANES:] = low
    gather_p[reach] = sums_row(masked(0, rows))
    near_start(gather_p, 0)

    mom1_load.wait()
    mom2_load.wait()
    for at in range(0, rows, block):
        g = own_half[at : at + block]
        mom1[at : at + block] = 0.9 * mom1[at : at + block]
        mom2[at : at + block] = 0.999 * mom2[at : at + block]
        got_half[at : at + block] = 0.001 * (g * g)
    finish(gather_g, recv_sem)
    grad_sq = jnp.sum(jnp.sum(gather_g[...], axis=0), axis=1, keepdims=True)
    clip = jnp.minimum(1.0, 1.0 / jnp.sqrt(grad_sq))
    c1 = 1.0 - 0.9**20
    c2 = 1.0 / (1.0 - 0.999**20)
    tenth, clip_sq = 0.1 * clip, clip * clip
    halves = 2
    span = rows // halves
    y = None
    for h in range(halves):
        for at in range(h * span, (h + 1) * span, block):
            nf = mom1[at : at + block] + tenth * own_half[at : at + block]
            ns = mom2[at : at + block] + clip_sq * got_half[at : at + block]
            nf_ref[at : at + block] = nf
            ns_ref[at : at + block] = ns
            root = ns * c2
            root = root * lax.rsqrt(root)
            d = nf / (c1 * root + c1 * 1e-08) + 0.01 * par_ref[at : at + block]
            dir_ref[at : at + block] = d
            high, low = split(d * d)
            parts[at : at + block, :LANES] = high
            parts[at : at + block, LANES:] = low
        part = masked(h * span, span)
        y = part if y is None else y + part
    gather_u[reach] = sums_row(y)
    near_start(gather_u, 1)

    for at in range(0, rows, block):
        r = at + lax.broadcasted_iota(jnp.int32, (block, trow), 0)
        mt_ref[at : at + block, 0:trow] = as_mask((r > sr_row) & (r < er_row))
        mt_ref[at : at + block, trow : 2 * trow] = as_mask(r == sr_row)
        mt_ref[at : at + block, 2 * trow : 3 * trow] = as_mask(r == er_row)
    w_ref[...] = jnp.zeros_like(w_ref)

    near_arrive(gather_p, 0)
    param_sq = jnp.sum(gather_p[...], axis=0)
    for copy in swaps:
        copy.wait_send()
    finish(gather_g, send_sem)
    near_leave(gather_p, 0)
    near_arrive(gather_u, 1)
    update_sq = jnp.sum(gather_u[...], axis=0)
    both = (param_sq > 0) & (update_sq > 0)
    trust_row = jnp.where(both, jnp.sqrt(param_sq) / jnp.sqrt(jnp.where(both, update_sq, 1.0)), 1.0)
    trust = jnp.sum(jnp.where(eye, trust_row, 0.0), axis=1, keepdims=True)
    weights = (jnp.broadcast_to(trust, (tcol, LANES)), trust * start_w, trust * end_w)
    for slot, weight in enumerate(weights):
        high, low = split(weight)
        w_ref[slot * trow : slot * trow + tcol, :LANES] = high
        w_ref[slot * trow : slot * trow + tcol, LANES:] = low
    near_leave(gather_u, 1)


def apply_kernel(nf_ref, ns_ref, dir_ref, par_ref, mt_ref, w_ref, np_out, nf_out, ns_out, ap_out,
                 np_buf, ap_buf, sem, chunk_sem):
    rows = dir_ref.shape[0]
    early = [
        pltpu.make_async_copy(nf_ref, nf_out, sem.at[0]),
        pltpu.make_async_copy(ns_ref, ns_out, sem.at[1]),
    ]
    for copy in early:
        copy.start()
    chunks = chunk_sem.shape[1]
    block = rows // chunks
    late = []
    for i in range(chunks):
        part = pl.ds(i * block, block)
        t = jnp.dot(mt_ref[part], w_ref[...], preferred_element_type=F32)
        applied = (t[:, :LANES] + t[:, LANES:]) * dir_ref[part]
        ap_buf[part] = applied
        np_buf[part] = par_ref[part] - 0.01 * applied
        for j, (src, dst) in enumerate(((ap_buf, ap_out), (np_buf, np_out))):
            copy = pltpu.make_async_copy(src.at[part], dst.at[part], chunk_sem.at[j, i])
            copy.start()
            late.append(copy)
    for copy in early + late:
        copy.wait()


def shards(fsdp, replica, gradients, tensor_sizes, params, first_moment, second_moment):
    assert replica == 2
    n = fsdp * replica
    rows = params.shape[0] // LANES
    tcol = round_up(tensor_sizes.shape[0], 16)
    trow = round_up(tensor_sizes.shape[0], LANES)
    hbm = pl.BlockSpec(memory_space=pltpu.HBM)
    vmem = pl.BlockSpec(memory_space=pltpu.VMEM)
    flat = (rows, LANES)
    pieces = 4
    reach = -(-n // 16)
    mids = pl.pallas_call(
        functools.partial(lamb_kernel, fsdp, replica),
        out_shape=[
            pltpu.VMEM(flat, F32),
            pltpu.VMEM(flat, F32),
            pltpu.VMEM(flat, F32),
            pltpu.VMEM(flat, F32),
            pltpu.VMEM((rows, 3 * trow), BF16),
            pltpu.VMEM((3 * trow, 2 * LANES), BF16),
        ],
        in_specs=[hbm] * 5,
        out_specs=[vmem] * 6,
        scratch_shapes=[
            pltpu.VMEM((1, tensor_sizes.shape[0]), jnp.int32),
            pltpu.VMEM((1, trow), jnp.int32),
            pltpu.VMEM(flat, F32),
            pltpu.VMEM(flat, F32),
            pltpu.VMEM(flat, F32),
            pltpu.VMEM(flat, F32),
            pltpu.VMEM(flat, F32),
            pltpu.VMEM((3 * tcol, rows), BF16),
            pltpu.VMEM((rows, 2 * LANES), BF16),
            pltpu.VMEM((n, 1, LANES), F32),
            pltpu.VMEM((2 * reach + 1, 1, trow), F32),
            pltpu.VMEM((2 * reach + 1, 1, trow), F32),
            pltpu.SemaphoreType.DMA((5,)),
            pltpu.SemaphoreType.DMA((pieces,)),
            pltpu.SemaphoreType.DMA((pieces,)),
            pltpu.SemaphoreType.DMA((pieces,)),
            pltpu.SemaphoreType.DMA,
            pltpu.SemaphoreType.DMA,
            pltpu.SemaphoreType.DMA((2, 2 * reach + 1)),
            pltpu.SemaphoreType.DMA((2, 2 * reach + 1)),
            pltpu.SemaphoreType.REGULAR,
            pltpu.SemaphoreType.REGULAR,
        ],
        compiler_params=pltpu.CompilerParams(
            collective_id=0, has_side_effects=True, vmem_limit_bytes=24 * 1024 * 1024
        ),
    )(
        in_hbm(tensor_sizes.reshape(1, -1)),
        in_hbm(gradients.reshape(replica * rows, LANES)),
        in_hbm(params.reshape(flat)),
        in_hbm(first_moment.reshape(flat)),
        in_hbm(second_moment.reshape(flat)),
    )
    chunks = 4
    outs = pl.pallas_call(
        apply_kernel,
        out_shape=[jax.ShapeDtypeStruct(flat, F32)] * 4,
        in_specs=[vmem] * 6,
        out_specs=[hbm] * 4,
        scratch_shapes=[
            pltpu.VMEM(flat, F32),
            pltpu.VMEM(flat, F32),
            pltpu.SemaphoreType.DMA((2,)),
            pltpu.SemaphoreType.DMA((2, chunks)),
        ],
        compiler_params=pltpu.CompilerParams(vmem_limit_bytes=24 * 1024 * 1024),
    )(*mids)
    return tuple(out.reshape(-1) for out in outs)


def solution(mesh):
    flat = P(("fsdp", "replica"))
    return jax.shard_map(
        functools.partial(shards, mesh.shape["fsdp"], mesh.shape["replica"]),
        mesh=mesh,
        in_specs=(P("replica", "fsdp"), P(), flat, flat, flat),
        out_specs=(flat,) * 4,
        check_vma=False,
    )
```
